32 devices in a mesh: dp: 2 (over x), row: 4 (over y, core), col: 4 (over z).
Axes of the slice: x: 2, y: 2, z: 4, core: 2. Of those that a mesh axis runs over, the one named last changes fastest.
Arguments:
- hidden_in: bfloat16 [2048, 2048], P(('dp', 'row'), 'col'), may hold values from -6 to 6
- cotangent: bfloat16 [2048, 2048], P(('dp', 'row'), 'col'), may hold values from -6 to 6
- segment_ids: int32 [8, 256], P(('dp', 'col')), may hold values from 0 to 3, never falling along the last dimension, each value on 1 to 128 neighbouring positions
- w_qkv: bfloat16 [2048, 3, 2048], P('col', None, 'row'), may hold values from -0.125 to 0.125
- b_qkv: bfloat16 [3, 2048], P(None, 'row'), may hold values from -6 to 6
- w_fc1: bfloat16 [2048, 8192], P('col', 'row'), may hold values from -0.125 to 0.125
- b_fc1: bfloat16 [8192], P('row'), may hold values from -3 to 3
- w_dense: bfloat16 [2048, 2048], P('row', 'col'), may hold values from -1 to 1
- w_fc2: bfloat16 [8192, 2048], P('row', 'col'), may hold values from -0.0625 to 0.0625
- out_bias: bfloat16 [2048], P('col'), may hold values from -3 to 3
- ln_gain: bfloat16 [2048], P('col'), may hold values from 0.099609375 to 1.8984375
- ln_shift: bfloat16 [2048], P('col'), may hold values from -2 to 2
Outputs:
- output: bfloat16 [2048, 2048], P(('dp', 'row'), 'col')
- grad_input: float32 [2048, 2048], P(('dp', 'row'), 'col')
- grad_w_qkv: float32 [2048, 3, 2048], P('col', None, 'row')
- grad_b_qkv: float32 [3, 2048], P(None, 'row')
- grad_w_fc1: float32 [2048, 8192], P('col', 'row')
- grad_b_fc1: float32 [8192], P('row')
- grad_w_dense: float32 [2048, 2048], P('row', 'col')
- grad_w_fc2: float32 [8192, 2048], P('row', 'col')
- grad_out_bias: float32 [2048], P('col')
- grad_ln_gain: float32 [2048], P('col')
- grad_ln_shift: float32 [2048], P('col')
The draws below stay inside these ranges and needn't reach their ends.
Inputs may be any that keep to these rules, and one draw needn't show every extreme that they name: `segment_ids`: segment ids never fall along a packed row; each id 0 to 3 covers 1 to 128 consecutive tokens of the row.
All inputs are finite; a program needn't handle non-finite values.
Results may differ from the reference program's by a relative error of at most 0.004.
The reference program's roundings to bfloat16 on the way count: a program that leaves them out, or rounds other values in their place, can miss the bound.
Values may be sent and summed in bfloat16 or wider, within the bound.
A program may use at most 256 MiB of HBM per device.

```python
import math
import jax
import jax.numpy as jnp
import numpy as np
from jax import lax

D = 2048
HEADS = 32
HEAD_DIM = 64
ROT = 32
FF = 8192
SEQ = 256
SEQS = 8
TOKENS = 2048


def draw_b_qkv(key, part):
    base_key = jax.random.fold_in(key, 11)
    return jnp.clip(0.5 * jax.random.normal(base_key, (3, D), jnp.float32), -3.0, 3.0).astype(jnp.bfloat16)


def shard_levels(key, shape, shards, least, high):
    factor_of, own = 1.0, jax.random.fold_in(key, 6)
    for dim, parts in shards:
        draws = jnp.exp(jax.random.uniform(jax.random.fold_in(own, dim), (parts,), jnp.float32, least / len(shards), high / len(shards)))
        factor_of = factor_of * jnp.repeat(draws, shape[dim] // parts).reshape([-1 if axis == dim else 1 for axis in range(len(shape))])
    return factor_of


def split_up(count, total, reach, slope):
    loads = [(1 << 20) // math.isqrt(grade ** slope) + 1 for grade in range(2, count + 1)]
    rest, counts = total - reach - (count - 1), [1] * (count - 1)
    while rest > 0:
        candidates = [i for i in range(count - 1) if counts[i] < reach]
        whole, left = sum([loads[i] for i in candidates]), rest
        for i in candidates:
            extra = min(reach - counts[i], max(1, left * loads[i] // whole), rest)
            counts[i] = counts[i] + extra
            rest = rest - extra
    return np.array([reach] + counts)


def ragged_sizes(own_key, number_of, total, reach, lean):
    if number_of == 2:
        one = jax.random.randint(own_key, (), max(1, total - reach), min(reach, total - 1) + 1)
        return jnp.stack([one, total - one])
    lengths = jnp.asarray(split_up(number_of, total, reach, lean), jnp.int32)
    twos = (number_of - 1) // 2
    donor, taker = lengths[1:1 + 2 * twos:2], lengths[2:2 + 2 * twos:2]
    room = jnp.minimum(donor - 1, reach - taker)
    shifted = jax.random.randint(jax.random.fold_in(own_key, 1), (twos,), 0, 1 << 20) % (room + 1)
    lengths = lengths.at[1:1 + 2 * twos:2].set(donor - shifted).at[2:2 + 2 * twos:2].set(taker + shifted)
    return lengths[jax.random.permutation(jax.random.fold_in(own_key, 2), number_of)]


def noise(key, shape, deviation, reach, shards=(), kind=jnp.bfloat16):
    array = jax.random.normal(key, shape, jnp.float32) * deviation
    if len(shards) > 0:
        array = shard_levels(key, shape, shards, -0.22, 0.18) * array
    return jnp.clip(array, min=-reach, max=reach).astype(kind)


def setup_inputs(seed: int = 0) -> dict:
    arg_keys = jax.random.split(jax.random.key(seed), 13)
    hidden_in = noise(arg_keys[0], (TOKENS, D), 1.0, 6.0, ((0, 8), (1, 4)))
    cotangent = noise(arg_keys[1], (TOKENS, D), 1.0, 6.0, ((0, 8), (1, 4)))
    segment_ids = jax.vmap(lambda own: jnp.searchsorted(jnp.cumsum(ragged_sizes(own, 4, SEQ, SEQ // 2, 0)), jnp.arange(SEQ), side="right"))(jax.random.split(arg_keys[2], SEQS)).reshape((SEQS, SEQ)).astype(jnp.int32)
    w_qkv = noise(arg_keys[3], (D, 3, D), D ** -0.5, 0.125, ((0, 4), (2, 4)))
    b_qkv = draw_b_qkv(jax.random.fold_in(arg_keys[12], 71), 0)
    w_fc1 = noise(arg_keys[5], (D, FF), D ** -0.5, 0.125, ((0, 4), (1, 4)))
    b_fc1 = noise(arg_keys[6], (FF,), 0.5, 3.0, ((0, 4),))
    w_dense = noise(arg_keys[7], (D, D), (D // 64) ** -0.5, 1.0, ((0, 4), (1, 4)))
    w_fc2 = noise(arg_keys[8], (FF, D), FF ** -0.5, 0.0625, ((0, 4), (1, 4)))
    out_bias = noise(arg_keys[9], (D,), 0.5, 3.0, ((0, 4),))
    ln_gain = jnp.clip(1.0 + 0.18 * jax.random.normal(arg_keys[10], (D,), jnp.float32), 0.099609375, 1.8984375).astype(jnp.bfloat16)
    ln_shift = noise(arg_keys[11], (D,), 0.3, 2.0, ((0, 4),))
    return {"hidden_in": hidden_in, "cotangent": cotangent, "segment_ids": segment_ids, "w_qkv": w_qkv, "b_qkv": b_qkv, "w_fc1": w_fc1, "b_fc1": b_fc1, "w_dense": w_dense, "w_fc2": w_fc2, "out_bias": out_bias, "ln_gain": ln_gain, "ln_shift": ln_shift}


epsilon = 1e-05
masked_score = -1e+30
highest = lax.Precision.HIGHEST

@jax.custom_vjp
def low(v):
    return lax.optimization_barrier(v.astype(jnp.bfloat16)).astype(jnp.float32)

@jax.custom_vjp
def low_back(v):
    return v

def low_keep(v):
    return (low(v), None)

def low_pass(kept, grad):
    return (grad,)

def back_keep(v):
    return (v, None)

def back_low(kept, grad):
    return (low(grad),)
low.defvjp(low_keep, low_pass)
low_back.defvjp(back_keep, back_low)

def rotary_tables(segments):
    length = segments.shape[0]
    position = jnp.arange(length, dtype=jnp.int32)
    boundary = jnp.concatenate([jnp.ones((1,), dtype=bool), segments[1:] != segments[:-1]])
    segment_start = lax.cummax(jnp.where(boundary, position, 0), axis=0)
    offset = (position - segment_start).astype(jnp.float32)
    half_width = ROT // 2
    inverse = 10000.0 ** (-(2.0 * jnp.arange(half_width, dtype=jnp.float32)) / ROT)
    angles = offset[:, None] * inverse[None, :]
    return (jnp.cos(angles)[:, None, :], jnp.sin(angles)[:, None, :])

def rotate(tensor, cosine, sine):
    half_width = ROT // 2
    leading = tensor[..., :half_width]
    trailing = tensor[..., half_width:ROT]
    return jnp.concatenate([leading * cosine - trailing * sine, trailing * cosine + leading * sine, tensor[..., ROT:]], axis=-1)

def attend(head_item):
    projected, segments = head_item
    cosine, sine = rotary_tables(segments)
    queries = low(rotate(projected[:, 0], cosine, sine))
    key_heads = low(rotate(projected[:, 1], cosine, sine))
    values = low(projected[:, 2])
    position = jnp.arange(segments.shape[0], dtype=jnp.int32)
    allowed = (segments[:, None] == segments[None, :]) & (position[:, None] >= position[None, :])
    scores = low_back(jnp.einsum('qhd,khd->hqk', queries, key_heads, precision=highest) * HEAD_DIM ** (-0.5))
    scores = jnp.where(allowed[None], scores, masked_score)
    peak_score = lax.optimization_barrier(jnp.max(scores, axis=-1, keepdims=True))
    exponentials = jnp.exp(scores - peak_score)
    probabilities = low(exponentials / lax.optimization_barrier(jnp.sum(exponentials, axis=-1, keepdims=True)))
    attn_mixed = jnp.einsum('hqk,khd->qhd', probabilities, values, precision=highest)
    return attn_mixed.reshape(attn_mixed.shape[0], HEADS * HEAD_DIM)

def block_layer(inputs, segments, w_qkv, b_qkv, w_fc1, b_fc1, w_dense, w_fc2, out_bias, ln_gain, ln_shift):
    row_mean = lax.optimization_barrier(jnp.mean(inputs, axis=-1, keepdims=True))
    centred = inputs - row_mean
    variance = lax.optimization_barrier(jnp.mean(centred * centred, axis=-1, keepdims=True))
    normed = low(centred * lax.rsqrt(variance + epsilon) * ln_gain + ln_shift)
    projected = low_back(jnp.dot(normed, w_qkv.reshape(D, 3 * D), precision=highest, preferred_element_type=jnp.float32) + b_qkv.reshape(3 * D))
    hidden_pre = low_back(jnp.dot(normed, w_fc1, precision=highest, preferred_element_type=jnp.float32) + b_fc1)
    activated = low(low_back(jax.nn.gelu(hidden_pre, approximate=True)))
    group_seqs = segments.shape[0]
    projected = projected.reshape(group_seqs, SEQ, 3, HEADS, HEAD_DIM)
    attn_mixed = lax.map(jax.checkpoint(attend), (projected, segments))
    attn_mixed = low(low_back(attn_mixed.reshape(group_seqs * SEQ, D)))
    return inputs + jnp.dot(attn_mixed, w_dense, precision=highest, preferred_element_type=jnp.float32) + jnp.dot(activated, w_fc2, precision=highest, preferred_element_type=jnp.float32) + out_bias

def reference(hidden_in, cotangent, segment_ids, w_qkv, b_qkv, w_fc1, b_fc1, w_dense, w_fc2, out_bias, ln_gain, ln_shift):
    group_seqs = math.gcd(max(1, 4096 // SEQ), SEQS)
    groups = SEQS // group_seqs
    parameters = tuple((a.astype(jnp.float32) for a in (w_qkv, b_qkv, w_fc1, b_fc1, w_dense, w_fc2, out_bias, ln_gain, ln_shift)))
    input_groups = hidden_in.astype(jnp.float32).reshape(groups, group_seqs * SEQ, D)
    cotangent_groups = cotangent.astype(jnp.float32).reshape(groups, group_seqs * SEQ, D)
    segment_groups = segment_ids.reshape(groups, group_seqs, SEQ)

    def group_step(summed, group_item):
        inputs, grad_out, segments = group_item
        result, pullback = jax.vjp(lambda block_in, *weights: block_layer(block_in, segments, *weights), inputs, *parameters)
        gradients = pullback(grad_out)
        summed = tuple((a + b for a, b in zip(summed, gradients[1:])))
        return (summed, (result.astype(jnp.bfloat16), gradients[0]))
    starting = tuple((jnp.zeros_like(p) for p in parameters))
    summed, (outputs, grad_inputs) = lax.scan(group_step, starting, (input_groups, cotangent_groups, segment_groups))
    return (outputs.reshape(TOKENS, D), grad_inputs.reshape(TOKENS, D), summed[0], summed[1], summed[2], summed[3], summed[4], summed[5], summed[6], summed[7], summed[8])
```

```python
import functools
import math

import jax
import jax.numpy as jnp
from jax import lax
from jax.experimental import pallas as pl
from jax.experimental.pallas import tpu as pltpu
from jax.sharding import PartitionSpec as P

HEAD_DIM = 64
ROT = 32
epsilon = 1e-05
masked_score = -1e30
f32 = jnp.float32
bf16 = jnp.bfloat16
C0 = math.sqrt(2.0 / math.pi)
C1 = 0.044715


def dot(a, b, ca, cb):
    return lax.dot_general(a, b, (((ca,), (cb,)), ((), ())), preferred_element_type=f32)


def rotary_tables(segments):
    length = segments.shape[1]
    position = jnp.arange(length, dtype=jnp.int32)
    boundary = jnp.concatenate(
        [jnp.ones((segments.shape[0], 1), dtype=bool), segments[:, 1:] != segments[:, :-1]], axis=1
    )
    segment_start = lax.cummax(jnp.where(boundary, position[None], 0), axis=1)
    offset = (position[None] - segment_start).astype(f32)
    half_width = ROT // 2
    inverse = 10000.0 ** (-(2.0 * jnp.arange(half_width, dtype=f32)) / ROT)
    angles = offset[..., None] * inverse
    cosine, sine = jnp.cos(angles), jnp.sin(angles)
    zero = jnp.zeros_like(sine)
    rest = jnp.zeros(angles.shape[:2] + (HEAD_DIM - ROT,), f32)
    own = jnp.concatenate([cosine, cosine, rest + 1.0], axis=-1)
    above = jnp.concatenate([-sine, zero, rest], axis=-1)
    below = jnp.concatenate([zero, sine, rest], axis=-1)
    return [jnp.concatenate([t, t], axis=-1) for t in (own, above, below)]


def remote(src, dst, send, recv, where):
    return pltpu.make_async_remote_copy(
        src_ref=src, dst_ref=dst, send_sem=send, recv_sem=recv, device_id=where, device_id_type=pl.DeviceIdType.MESH
    )


def greet(others):
    barrier = pltpu.get_barrier_semaphore()
    count = 0
    for cond, where in others:
        if cond is True:
            pl.semaphore_signal(barrier, inc=1, device_id=where, device_id_type=pl.DeviceIdType.MESH)
            count += 1
        else:

            @pl.when(cond)
            def _():
                pl.semaphore_signal(barrier, inc=1, device_id=where, device_id_type=pl.DeviceIdType.MESH)

            count += cond.astype(jnp.int32)
    pl.semaphore_wait(barrier, count)


def gather_kernel(both_ref, all_ref, lsem, zs, zr, xs, xr, ys, yr, cs, cr):
    _, n, dz = both_ref.shape
    nc = all_ref.shape[2] // dz
    nr = lax.axis_size("row")
    x, r, z = lax.axis_index("dp"), lax.axis_index("row"), lax.axis_index("col")
    xp, yp, cp = {"dp": 1 - x}, {"row": lax.rem(r + 2, nr)}, {"row": r + 1 - 2 * lax.rem(r, 2)}
    left, right = {"col": z - 1}, {"col": z + 1}
    greet([(True, xp), (True, yp), (True, cp), (z > 0, left), (z < nc - 1, right)])

    def item(g, zz):
        return all_ref.at[:, pl.ds(pl.multiple_of(g * n, n), n), pl.ds(pl.multiple_of(zz * dz, dz), dz)]

    rp, rc = lax.rem(r + 2, nr), r + 1 - 2 * lax.rem(r, 2)
    rcp = lax.rem(rc + 2, nr)
    mine = [x * nr + r, (1 - x) * nr + r, x * nr + rp, (1 - x) * nr + rp]
    theirs = [x * nr + rc, (1 - x) * nr + rc, x * nr + rcp, (1 - x) * nr + rcp]

    def each(body):
        for s in range(nc):
            for zz in [z] if s == 0 else [z - s, z + s]:
                if s == 0:
                    body(s, zz)
                else:

                    @pl.when((zz >= 0) & (zz < nc))
                    def _():
                        body(s, zz)

    keep = pltpu.make_async_copy(both_ref, item(mine[0], z), lsem)
    keep.start()

    def to_left(src, zz):
        return remote(src, item(mine[0], zz), zs.at[0, zz], zr.at[zz], left)

    def to_right(src, zz):
        return remote(src, item(mine[0], zz), zs.at[1, zz], zr.at[zz], right)

    def to_x(k, src, g, zz):
        return remote(src, item(g, zz), xs.at[k, zz], xr.at[k, zz], xp)

    def to_y(k, src, g, zz):
        return remote(src, item(g, zz), ys.at[k, zz], yr.at[k, zz], yp)

    def to_core(k, src, g, zz):
        return remote(src, item(g, zz), cs.at[k, zz], cr.at[k, zz], cp)

    def first(s, zz):
        src = both_ref if s == 0 else item(mine[0], zz)
        if s > 0:
            to_left(src, zz).wait_recv()

        @pl.when((zz >= z) & (z > 0))
        def _():
            to_left(src, zz).start()

        @pl.when((zz <= z) & (z < nc - 1))
        def _():
            to_right(src, zz).start()

        to_x(0, src, mine[0], zz).start()
        to_y(0, src, mine[0], zz).start()
        to_core(0, src, mine[0], zz).start()

    each(first)

    def second(s, zz):
        even = lax.rem(zz, 2) == 0
        a, b = item(mine[1], zz), item(mine[2], zz)
        to_x(0, a, mine[1], zz).wait_recv()

        @pl.when(even)
        def _():
            to_y(1, a, mine[1], zz).start()

        to_core(1, a, mine[1], zz).start()
        to_y(0, b, mine[2], zz).wait_recv()

        @pl.when(jnp.logical_not(even))
        def _():
            to_x(1, b, mine[2], zz).start()

        to_core(2, b, mine[2], zz).start()

    each(second)

    def third(s, zz):
        even = lax.rem(zz, 2) == 0
        d = item(mine[3], zz)

        @pl.when(even)
        def _():
            to_y(1, d, mine[3], zz).wait_recv()

        @pl.when(jnp.logical_not(even))
        def _():
            to_x(1, d, mine[3], zz).wait_recv()

        to_core(3, d, mine[3], zz).start()

    each(third)
    keep.wait()

    def last(s, zz):
        even = lax.rem(zz, 2) == 0
        src = both_ref
        for k in range(4):
            to_core(k, src, theirs[k], zz).wait_recv()
            to_core(k, src, theirs[k], zz).wait_send()
        to_x(0, src, mine[0], zz).wait_send()
        to_y(0, src, mine[0], zz).wait_send()

        @pl.when(even)
        def _():
            to_y(1, src, mine[1], zz).wait_send()

        @pl.when(jnp.logical_not(even))
        def _():
            to_x(1, src, mine[2], zz).wait_send()

        @pl.when((zz >= z) & (z > 0))
        def _():
            to_left(src, zz).wait_send()

        @pl.when((zz <= z) & (z < nc - 1))
        def _():
            to_right(src, zz).wait_send()

    each(last)


def tail_kernel(
    D, part_ref, gpart_ref, both_ref, stat_ref, gain_ref, bias_ref,
    out_ref, gin_ref, vec_ref,
    cbuf, b1, b2, zbuf, vbuf, cs, cr, s1s, s1r, s2s, s2r, zs, zr, vs, vr,
):
    _, n, dz = both_ref.shape
    nd, nr, nc = lax.axis_size("dp"), lax.axis_size("row"), lax.axis_size("col")
    x, r, z = lax.axis_index("dp"), lax.axis_index("row"), lax.axis_index("col")
    y, c = r // 2, lax.rem(r, 2)
    xp, yp, cp = {"dp": 1 - x}, {"row": lax.rem(r + 2, nr)}, {"row": r + 1 - 2 * c}
    along_z = [{"col": lax.rem(z + k, nc)} for k in range(1, nc)]
    me = x * nr + r
    npl = nd * nr
    plane = []
    for k in range(1, npl):
        g = lax.rem(me + k, npl)
        plane.append({"dp": g // nr, "row": lax.rem(g, nr)})
    greet([(True, w) for w in along_z + plane])

    def rows(xx, yy, cc):
        return pl.ds(pl.multiple_of((xx * nr + yy * 2 + cc) * n, n), n)

    arrays = [part_ref, gpart_ref]
    places = [(x, y), (1 - x, y), (x, 1 - y), (1 - x, 1 - y)]

    core = [[remote(arrays[a].at[rows(*places[k], 1 - c)], cbuf.at[a, k], cs.at[a, k], cr.at[a, k], cp) for k in range(4)] for a in range(2)]
    order = [(0, 1), (0, 3), (1, 2), (1, 3), (0, 2), (1, 1), (0, 0), (1, 0)]
    for a, k in order:
        core[a][k].start()

    def chip_sum(a, k):
        core[a][k].wait_recv()
        cbuf[a, k] = cbuf[a, k] + arrays[a][rows(*places[k], c), :]

    across = [xp, yp]
    far = [1, 2]
    one = [[None, None], [None, None]]
    for a in range(2):
        for j, k in enumerate([far[a], 3]):
            one[a][j] = remote(cbuf.at[a, k], b1.at[a, j], s1s.at[a, j], s1r.at[a, j], across[a])
    for a, k in order[:4]:
        chip_sum(a, k)
        one[a][0 if k == far[a] else 1].start()
    for a, k in order[4:]:
        chip_sum(a, k)
    two = []
    for a in range(2):
        k = far[1 - a]
        one[a][1].wait_recv()
        b1[a, 1] = b1[a, 1] + cbuf[a, k]
        two.append(remote(b1.at[a, 1], b2.at[a], s2s.at[a], s2r.at[a], across[1 - a]))
        two[a].start()
    for a in range(2):
        one[a][0].wait_recv()
        cbuf[a, 0] = cbuf[a, 0] + b1[a, 0]
    hid = both_ref[0].astype(f32)
    mean, inv = stat_ref[:, 0:1], stat_ref[:, 1:2]
    xhat = (hid - mean) * inv
    two[1].wait_recv()
    gn = cbuf[1, 0] + b2[1]
    gnx = gn * xhat
    g = gn * gain_ref[...]
    lane = lax.broadcasted_iota(jnp.int32, (n, 128), 1)
    sums = jnp.where(lane == 0, jnp.sum(g, axis=1, keepdims=True), jnp.sum(g * xhat, axis=1, keepdims=True))
    zbuf[z] = sums.T[:8]
    line = lax.broadcasted_iota(jnp.int32, (8, dz), 0)
    vbuf[me] = jnp.where(
        line == 0, jnp.sum(gnx, axis=0, keepdims=True), jnp.where(line == 1, jnp.sum(gn, axis=0, keepdims=True), 0.0)
    )
    zc = [remote(zbuf.at[z], zbuf.at[z], zs.at[k], zr.at[k], w) for k, w in enumerate(along_z)]
    for copy in zc:
        copy.start()
    vc = [remote(vbuf.at[me], vbuf.at[me], vs.at[k], vr.at[k], w) for k, w in enumerate(plane)]
    for copy in vc:
        copy.start()
    two[0].wait_recv()
    out_ref[...] = (hid + (cbuf[0, 0] + b2[0]) + bias_ref[...]).astype(bf16)
    for copy in zc:
        copy.wait()
    total = zbuf[0]
    for k in range(1, nc):
        total += zbuf[k]
    both = jnp.concatenate([total] * (128 // 8), axis=0).T
    gin_ref[...] = both_ref[1].astype(f32) + inv * (g - both[:, 0:1] / D - xhat * (both[:, 1:2] / D))
    for copy in vc:
        copy.wait()
    total = vbuf[0]
    for k in range(1, npl):
        total += vbuf[k]
    vec_ref[...] = total
    for a, k in order:
        core[a][k].wait_send()
    for a in range(2):
        one[a][0].wait_send()
        one[a][1].wait_send()
        two[a].wait_send()


def norm_kernel(both_ref, gain_ref, shift_ref, normed_ref, stat_ref):
    hid = both_ref[0].astype(f32)
    D = hid.shape[1]
    mean = jnp.sum(hid, axis=1, keepdims=True) / D
    cen = hid - mean
    inv = lax.rsqrt(jnp.sum(cen * cen, axis=1, keepdims=True) / D + epsilon)
    normed_ref[...] = (cen * inv * gain_ref[...] + shift_ref[...]).astype(bf16)
    lane = lax.broadcasted_iota(jnp.int32, stat_ref.shape, 1)
    stat_ref[...] = jnp.where(lane == 0, mean, inv)


def attn_kernel(
    normed_ref, cot_ref, wq_ref, wd_ref, bq_ref, own_ref, above_ref, below_ref, srow_ref, scol_ref,
    part_ref, gpart_ref, dwq_ref, dwd_ref, dbq_ref,
):
    s = pl.program_id(0)
    z = lax.axis_index("col")
    nz, aw, dz = wd_ref.shape
    seq = normed_ref.shape[0]
    heads = aw // HEAD_DIM
    local = pl.ds(pl.multiple_of(z * dz, dz), dz)
    wide = lambda r: jnp.concatenate([r[0]] * (aw // 128), axis=1)
    own, above, below = wide(own_ref), wide(above_ref), wide(below_ref)

    def rot(t):
        return t * own + pltpu.roll(t, aw - ROT // 2, 1) * above + pltpu.roll(t, ROT // 2, 1) * below

    def unrot(t):
        return t * own - pltpu.roll(t, aw - ROT // 2, 1) * above - pltpu.roll(t, ROT // 2, 1) * below

    proj = dot(normed_ref[...], wq_ref[...], 1, 0) + bq_ref[...]
    q = rot(proj[:, :aw]).astype(bf16)
    k = rot(proj[:, aw : 2 * aw]).astype(bf16)
    v = proj[:, 2 * aw :].astype(bf16)
    gm = jnp.zeros((seq, aw), f32)
    for i in range(nz):
        gm += dot(cot_ref[:, i * dz : (i + 1) * dz], wd_ref[i], 1, 1)
    gm = gm.astype(bf16)
    rows = lax.broadcasted_iota(jnp.int32, (seq, seq), 0)
    cols = lax.broadcasted_iota(jnp.int32, (seq, seq), 1)
    allowed = (scol_ref[0] == srow_ref[0]) & (rows >= cols)
    head_of = lax.broadcasted_iota(jnp.int32, (seq, aw), 1) // HEAD_DIM
    scale = HEAD_DIM ** (-0.5)
    mixed = jnp.zeros((seq, aw), f32)
    gq = jnp.zeros((seq, aw), f32)
    gk = jnp.zeros((seq, aw), f32)
    gv = jnp.zeros((seq, aw), f32)
    zero = jnp.zeros((seq, aw), bf16)
    for h in range(heads):
        mine = head_of == h
        qh = jnp.where(mine, q, zero)
        kh = jnp.where(mine, k, zero)
        vh = jnp.where(mine, v, zero)
        gh = jnp.where(mine, gm, zero)
        scores = jnp.where(allowed, dot(qh, k, 1, 1) * scale, masked_score)
        peak = jnp.max(scores, axis=1, keepdims=True)
        ex = jnp.exp(scores - peak)
        soft = ex * (1.0 / jnp.sum(ex, axis=1, keepdims=True))
        probs = soft.astype(bf16)
        mixed += dot(probs, vh, 1, 0)
        gp = dot(gh, v, 1, 1)
        centre = jnp.sum(soft * gp, axis=1, keepdims=True)
        gs = (soft * (gp - centre)).astype(bf16)
        gq += dot(gs, kh, 1, 0)
        gk += dot(gs, qh, 0, 0)
        gv += dot(probs, gh, 0, 0)
    mixed = mixed.astype(bf16)
    g = jnp.concatenate([unrot(gq * scale), unrot(gk * scale), gv], axis=1).astype(bf16)
    cot_loc = cot_ref[:, local]
    normed_loc = normed_ref[:, local]
    part_ref[...] = dot(mixed, wd_ref[z], 1, 0)
    gpart_ref[...] = dot(g, wq_ref[local, :], 1, 1)

    @pl.when(s == 0)
    def _():
        dwq_ref[...] = jnp.zeros_like(dwq_ref)
        dwd_ref[...] = jnp.zeros_like(dwd_ref)
        dbq_ref[...] = jnp.zeros_like(dbq_ref)

    dwq_ref[...] += dot(normed_loc, g, 0, 0)
    dwd_ref[...] += dot(mixed, cot_loc, 0, 0)
    dbq_ref[...] += jnp.sum(g.astype(f32), axis=0, keepdims=True)


def mlp_kernel(
    normed_ref, cot_ref, w1_ref, w2_ref, b1_ref, part_in, gpart_in,
    part_ref, gpart_ref, dw1_ref, dw2_ref, db1_ref, act_s, gh_s,
):
    s = pl.program_id(0)
    z = lax.axis_index("col")
    nz, fw, dz = w2_ref.shape
    tb = normed_ref.shape[0]
    local = pl.ds(pl.multiple_of(z * dz, dz), dz)
    fb = 256
    for j in range(fw // fb):
        fs = slice(j * fb, (j + 1) * fb)
        u = dot(normed_ref[...], w1_ref[:, fs], 1, 0) + b1_ref[:, fs]
        ga = jnp.zeros((tb, fb), f32)
        for i in range(nz):
            ga += dot(cot_ref[:, i * dz : (i + 1) * dz], w2_ref[i, fs, :], 1, 1)
        ga = ga.astype(bf16).astype(f32)
        u2 = u * u
        t = jnp.tanh(C0 * (u + C1 * (u2 * u)))
        cdf = 0.5 * (1.0 + t)
        act_s[:, fs] = (u * cdf).astype(bf16)
        slope = cdf + (0.5 * u) * (1.0 - t * t) * (C0 * (1.0 + (3.0 * C1) * u2))
        gh_s[:, fs] = (slope * ga).astype(bf16)
    act, gh = act_s[...], gh_s[...]
    cot_loc = cot_ref[:, local]
    normed_loc = normed_ref[:, local]
    part_ref[...] = part_in[...] + dot(act, w2_ref[z], 1, 0)
    gpart_ref[...] = gpart_in[...] + dot(gh, w1_ref[local, :], 1, 1)

    @pl.when(s == 0)
    def _():
        dw1_ref[...] = jnp.zeros_like(dw1_ref)
        dw2_ref[...] = jnp.zeros_like(dw2_ref)
        db1_ref[...] = jnp.zeros_like(db1_ref)

    dw1_ref[...] += dot(normed_loc, gh, 0, 0)
    dw2_ref[...] += dot(act, cot_loc, 0, 0)
    db1_ref[...] += jnp.sum(gh.astype(f32), axis=0, keepdims=True)


def shape(s, d):
    return jax.ShapeDtypeStruct(s, d)


def whole(s):
    return pl.BlockSpec(s, lambda i: (0,) * len(s))


def shards(hidden_in, cotangent, segment_ids, w_qkv, b_qkv, w_fc1, b_fc1, w_dense, w_fc2, out_bias, ln_gain, ln_shift):
    nd, nr, nc = lax.axis_size("dp"), lax.axis_size("row"), lax.axis_size("col")
    x, z = lax.axis_index("dp"), lax.axis_index("col")
    seq_len = segment_ids.shape[1]
    nloc, dz = hidden_in.shape
    D = dz * nc
    T = nloc * nd * nr
    nseq = T // seq_len
    aw = w_qkv.shape[2] // nd
    fw = w_fc1.shape[1] // nd
    half = lambda w, n, axis: lax.dynamic_slice_in_dim(w, x * n, n, axis)

    both = jnp.stack([hidden_in, cotangent])
    dma = pltpu.SemaphoreType.DMA
    pair = pl.pallas_call(
        gather_kernel,
        in_specs=[pl.BlockSpec(memory_space=pl.ANY)],
        out_specs=pl.BlockSpec(memory_space=pl.ANY),
        out_shape=shape((2, T, D), bf16),
        scratch_shapes=[
            dma, dma((2, nc)), dma((nc,)), dma((2, nc)), dma((2, nc)), dma((2, nc)), dma((2, nc)), dma((4, nc)), dma((4, nc)),
        ],
        compiler_params=pltpu.CompilerParams(collective_id=0, has_side_effects=True),
        name="gather",
    )(both)
    segs = lax.all_gather(segment_ids, ("dp", "col"), axis=0, tiled=True)
    gain_all, shift_all = lax.all_gather(jnp.stack([ln_gain, ln_shift]), "col", axis=1, tiled=True).astype(f32)

    wq = half(w_qkv, aw, 2).reshape(dz, 3 * aw)
    wd = half(w_dense, aw, 0)
    w1 = half(w_fc1, fw, 1)
    w2 = half(w_fc2, fw, 0)
    bq = half(b_qkv, aw, 1).astype(f32).reshape(1, 3 * aw)
    b1 = half(b_fc1, fw, 0).astype(f32).reshape(1, fw)
    wq_all = lax.all_gather(wq, "col", axis=0, tiled=True)
    wd_all = lax.all_gather(wd, "col", axis=0)
    nchunk = 2
    fc = fw // nchunk
    w1_all = [lax.all_gather(w1[:, i * fc : (i + 1) * fc], "col", axis=0, tiled=True) for i in range(nchunk)]
    w2_all = [lax.all_gather(w2[i * fc : (i + 1) * fc], "col", axis=0) for i in range(nchunk)]

    nb = min(256, seq_len)
    normed, stat = pl.pallas_call(
        norm_kernel,
        grid=(T // nb,),
        in_specs=[pl.BlockSpec((1, nb, D), lambda i: (0, i, 0)), whole((1, D)), whole((1, D))],
        out_specs=[pl.BlockSpec((nb, D), lambda i: (i, 0)), pl.BlockSpec((nb, 128), lambda i: (i, 0))],
        out_shape=[shape((T, D), bf16), shape((T, 128), f32)],
        name="norm",
    )(pair, gain_all.reshape(1, D), shift_all.reshape(1, D))

    tables = rotary_tables(segs)
    cot_blk = lambda n: pl.BlockSpec((None, n, D), lambda i: (1, i, 0))
    blk = lambda n, w: pl.BlockSpec((n, w), lambda i: (i, 0))
    seq_blk = lambda a, b: pl.BlockSpec((1, a, b), lambda i: (i, 0, 0))
    part, gpart, dwq, dwd, dbq = pl.pallas_call(
        attn_kernel,
        grid=(nseq,),
        in_specs=[
            blk(seq_len, D), cot_blk(seq_len), whole((D, 3 * aw)), whole((nc, aw, dz)), whole((1, 3 * aw)),
            seq_blk(seq_len, 128), seq_blk(seq_len, 128), seq_blk(seq_len, 128), seq_blk(1, seq_len), seq_blk(seq_len, 1),
        ],
        out_specs=[blk(seq_len, dz), blk(seq_len, dz), whole((dz, 3 * aw)), whole((aw, dz)), whole((1, 3 * aw))],
        out_shape=[
            shape((T, dz), f32), shape((T, dz), f32), shape((dz, 3 * aw), f32), shape((aw, dz), f32), shape((1, 3 * aw), f32),
        ],
        name="attn",
    )(normed, pair, wq_all, wd_all, bq, *tables, segs[:, None, :], segs[:, :, None])

    tb = 512
    dw1s, dw2s, db1s = [], [], []
    for i in range(nchunk):
        part, gpart, a, b, c = pl.pallas_call(
            mlp_kernel,
            grid=(T // tb,),
            in_specs=[
                blk(tb, D), cot_blk(tb), whole((D, fc)), whole((nc, fc, dz)), whole((1, fc)), blk(tb, dz), blk(tb, dz),
            ],
            out_specs=[blk(tb, dz), blk(tb, dz), whole((dz, fc)), whole((fc, dz)), whole((1, fc))],
            out_shape=[shape((T, dz), f32), shape((T, dz), f32), shape((dz, fc), f32), shape((fc, dz), f32), shape((1, fc), f32)],
            scratch_shapes=[pltpu.VMEM((tb, fc), bf16), pltpu.VMEM((tb, fc), bf16)],
            name="mlp",
        )(normed, pair, w1_all[i], w2_all[i], b1[:, i * fc : (i + 1) * fc], part, gpart)
        dw1s.append(a)
        dw2s.append(b)
        db1s.append(c)

    me = lax.axis_index(("dp", "row"))
    stat_l = lax.dynamic_slice_in_dim(stat, me * nloc, nloc, 0)
    vmem = pl.BlockSpec(memory_space=pltpu.VMEM)
    npl = nd * nr
    output, grad_input, vec = pl.pallas_call(
        functools.partial(tail_kernel, D),
        in_specs=[vmem] * 6,
        out_specs=[vmem] * 3,
        out_shape=[shape((nloc, dz), bf16), shape((nloc, dz), f32), shape((8, dz), f32)],
        scratch_shapes=[
            pltpu.VMEM((2, 4, nloc, dz), f32), pltpu.VMEM((2, 2, nloc, dz), f32), pltpu.VMEM((2, nloc, dz), f32),
            pltpu.VMEM((nc, 8, nloc), f32), pltpu.VMEM((npl, 8, dz), f32),
            dma((2, 4)), dma((2, 4)), dma((2, 2)), dma((2, 2)), dma((2,)), dma((2,)),
            dma((nc - 1,)), dma((nc - 1,)), dma((npl - 1,)), dma((npl - 1,)),
        ],
        compiler_params=pltpu.CompilerParams(collective_id=1, has_side_effects=True),
        name="tail",
    )(part, gpart, both, stat_l, ln_gain.astype(f32).reshape(1, dz), out_bias.astype(f32).reshape(1, dz))
    cot_loc = lax.dynamic_slice(pair, (1, 0, z * dz), (1, T, dz))[0]
    d_ob = jnp.sum(cot_loc.astype(f32), axis=0)

    ag = lambda a, axis: lax.all_gather(a, "dp", axis=axis, tiled=True)
    return (
        output,
        grad_input,
        ag(dwq.reshape(dz, 3, aw), 2),
        ag(dbq.reshape(3, aw), 1),
        ag(jnp.concatenate(dw1s, axis=1), 1),
        ag(jnp.concatenate(db1s, axis=1)[0], 0),
        ag(dwd, 0),
        ag(jnp.concatenate(dw2s, axis=0), 0),
        d_ob,
        vec[0],
        vec[1],
    )


def solution(mesh):
    in_specs = (
        P(("dp", "row"), "col"), P(("dp", "row"), "col"), P(("dp", "col"), None), P("col", None, "row"), P(None, "row"),
        P("col", "row"), P("row"), P("row", "col"), P("row", "col"), P("col"), P("col"), P("col"),
    )
    out_specs = (
        P(("dp", "row"), "col"), P(("dp", "row"), "col"), P("col", None, "row"), P(None, "row"), P("col", "row"), P("row"),
        P("row", "col"), P("row", "col"), P("col"), P("col"), P("col"),
    )
    return jax.shard_map(shards, mesh=mesh, in_specs=in_specs, out_specs=out_specs, check_vma=False)
```

```python
import functools
import math

import jax
import jax.numpy as jnp
from jax import lax
from jax.experimental import pallas as pl
from jax.experimental.pallas import tpu as pltpu
from jax.sharding import PartitionSpec as P

HEAD_DIM = 64
ROT = 32
epsilon = 1e-05
masked_score = -1e30
f32 = jnp.float32
bf16 = jnp.bfloat16
C0 = math.sqrt(2.0 / math.pi)
C1 = 0.044715


def dot(a, b, ca, cb):
    return lax.dot_general(a, b, (((ca,), (cb,)), ((), ())), preferred_element_type=f32)


def remote(src, dst, send, recv, where):
    return pltpu.make_async_remote_copy(
        src_ref=src, dst_ref=dst, send_sem=send, recv_sem=recv, device_id=where, device_id_type=pl.DeviceIdType.MESH
    )


def greet(others):
    barrier = pltpu.get_barrier_semaphore()
    count = 0
    for cond, where in others:
        if cond is True:
            pl.semaphore_signal(barrier, inc=1, device_id=where, device_id_type=pl.DeviceIdType.MESH)
            count += 1
        else:

            @pl.when(cond)
            def _():
                pl.semaphore_signal(barrier, inc=1, device_id=where, device_id_type=pl.DeviceIdType.MESH)

            count += cond.astype(jnp.int32)
    pl.semaphore_wait(barrier, count)


def gather_kernel(
    both_ref, wq_ref, wd_ref, small_ref, all_ref, wq_all, wd_all, small_all,
    lsem, zs, zr, xs, xr, ys, yr, cs, cr, as_, ar, ss, sr,
):
    _, n, dz = both_ref.shape
    nd, nr, nc = lax.axis_size("dp"), lax.axis_size("row"), wd_all.shape[0]
    aw = wd_all.shape[1]
    x, r, z = lax.axis_index("dp"), lax.axis_index("row"), lax.axis_index("col")
    rp, rc = lax.rem(r + 2, nr), r + 1 - 2 * lax.rem(r, 2)
    rcp = lax.rem(rc + 2, nr)
    xp, yp, cp = {"dp": 1 - x}, {"row": rp}, {"row": rc}
    left, right = {"col": z - 1}, {"col": z + 1}
    ns = nd * nc
    me = x * nc + z
    others = []
    for k in range(1, ns):
        o = lax.rem(me + k, ns)
        others.append({"dp": o // nc, "col": lax.rem(o, nc)})
    greet([(True, yp), (True, cp)] + [(True, o) for o in others])

    def item(g, zz):
        return all_ref.at[:, pl.ds(pl.multiple_of(g * n, n), n), pl.ds(pl.multiple_of(zz * dz, dz), dz)]

    mine = [x * nr + r, (1 - x) * nr + r, x * nr + rp, (1 - x) * nr + rp]
    theirs = [x * nr + rc, (1 - x) * nr + rc, x * nr + rcp, (1 - x) * nr + rcp]

    def each(body, steps=range(nc)):
        for s in steps:
            for zz in [z] if s == 0 else [z - s, z + s]:
                if s == 0:
                    body(s, zz)
                else:

                    @pl.when((zz >= 0) & (zz < nc))
                    def _():
                        body(s, zz)

    wd_own = wd_ref.at[pl.ds(pl.multiple_of(x * aw, aw), aw), :]
    wq_at = lambda zz: wq_all.at[pl.ds(pl.multiple_of(zz * dz, dz), dz), :]
    keeps = [
        pltpu.make_async_copy(both_ref, item(mine[0], z), lsem.at[0]),
        pltpu.make_async_copy(wq_ref, wq_at(z), lsem.at[1]),
        pltpu.make_async_copy(wd_own, wd_all.at[z], lsem.at[2]),
        pltpu.make_async_copy(small_ref, small_all.at[me], lsem.at[3]),
    ]
    tiny = [remote(small_ref, small_all.at[me], ss.at[k], sr.at[k], o) for k, o in enumerate(others)]

    def to_left(src, zz):
        return remote(src, item(mine[0], zz), zs.at[0, zz], zr.at[zz], left)

    def to_right(src, zz):
        return remote(src, item(mine[0], zz), zs.at[1, zz], zr.at[zz], right)

    def weights(d, own, zz):
        return [
            remote(wq_ref if own else wq_at(zz), wq_at(zz), as_.at[0, d, zz], ar.at[0, zz], [left, right][d]),
            remote(wd_own if own else wd_all.at[zz], wd_all.at[zz], as_.at[1, d, zz], ar.at[1, zz], [left, right][d]),
        ]

    def to_x(k, src, g, zz):
        return remote(src, item(g, zz), xs.at[k, zz], xr.at[k, zz], xp)

    def to_y(k, src, g, zz):
        return remote(src, item(g, zz), ys.at[k, zz], yr.at[k, zz], yp)

    def to_core(k, src, g, zz):
        return remote(src, item(g, zz), cs.at[k, zz], cr.at[k, zz], cp)

    def first(s, zz):
        src = both_ref if s == 0 else item(mine[0], zz)
        if s > 0:
            to_left(src, zz).wait_recv()

        @pl.when((zz >= z) & (z > 0))
        def _():
            to_left(src, zz).start()

        @pl.when((zz <= z) & (z < nc - 1))
        def _():
            to_right(src, zz).start()

        to_x(0, src, mine[0], zz).start()
        to_y(0, src, mine[0], zz).start()
        to_core(0, src, mine[0], zz).start()

    def pass_weights(s, zz):
        if s > 0:
            for copy in weights(0, False, zz):
                copy.wait_recv()

        @pl.when((zz >= z) & (z > 0))
        def _():
            for copy in weights(0, s == 0, zz):
                copy.start()

        @pl.when((zz <= z) & (z < nc - 1))
        def _():
            for copy in weights(1, s == 0, zz):
                copy.start()

    def second(s, zz):
        even = lax.rem(zz, 2) == 0
        a, b = item(mine[1], zz), item(mine[2], zz)
        to_x(0, a, mine[1], zz).wait_recv()

        @pl.when(even)
        def _():
            to_y(1, a, mine[1], zz).start()

        to_core(1, a, mine[1], zz).start()
        to_y(0, b, mine[2], zz).wait_recv()

        @pl.when(jnp.logical_not(even))
        def _():
            to_x(1, b, mine[2], zz).start()

        to_core(2, b, mine[2], zz).start()

    def third(s, zz):
        even = lax.rem(zz, 2) == 0
        d = item(mine[3], zz)

        @pl.when(even)
        def _():
            to_y(1, d, mine[3], zz).wait_recv()

        @pl.when(jnp.logical_not(even))
        def _():
            to_x(1, d, mine[3], zz).wait_recv()

        to_core(3, d, mine[3], zz).start()

    each(first, range(1))
    for copy in tiny + keeps:
        copy.start()
    each(first, range(1, nc))
    each(pass_weights, range(1))
    each(second)
    each(pass_weights, range(1, 2))
    each(third)
    each(pass_weights, range(2, nc))
    for copy in keeps:
        copy.wait()
    for copy in tiny:
        copy.wait()

    def last(s, zz):
        even = lax.rem(zz, 2) == 0
        src = both_ref
        for k in range(4):
            to_core(k, src, theirs[k], zz).wait_recv()
            to_core(k, src, theirs[k], zz).wait_send()
        to_x(0, src, mine[0], zz).wait_send()
        to_y(0, src, mine[0], zz).wait_send()

        @pl.when(even)
        def _():
            to_y(1, src, mine[1], zz).wait_send()

        @pl.when(jnp.logical_not(even))
        def _():
            to_x(1, src, mine[2], zz).wait_send()

        @pl.when((zz >= z) & (z > 0))
        def _():
            for copy in [to_left(src, zz)] + weights(0, True, zz):
                copy.wait_send()

        @pl.when((zz <= z) & (z < nc - 1))
        def _():
            for copy in [to_right(src, zz)] + weights(1, True, zz):
                copy.wait_send()

    each(last)


def tail_kernel(
    D, part_ref, gpart_ref, both_ref, stat_ref, gain_ref, bias_ref,
    out_ref, gin_ref, vec_ref,
    cbuf, b1, b2, zbuf, vbuf, cs, cr, s1s, s1r, s2s, s2r, zs, zr, vs, vr,
):
    _, n, dz = both_ref.shape
    nd, nr, nc = lax.axis_size("dp"), lax.axis_size("row"), lax.axis_size("col")
    x, r, z = lax.axis_index("dp"), lax.axis_index("row"), lax.axis_index("col")
    y, c = r // 2, lax.rem(r, 2)
    xp, yp, cp = {"dp": 1 - x}, {"row": lax.rem(r + 2, nr)}, {"row": r + 1 - 2 * c}
    along_z = [{"col": lax.rem(z + k, nc)} for k in range(1, nc)]
    me = x * nr + r
    npl = nd * nr
    plane = []
    for k in range(1, npl):
        g = lax.rem(me + k, npl)
        plane.append({"dp": g // nr, "row": lax.rem(g, nr)})
    greet([(True, w) for w in along_z + plane])

    def rows(xx, yy, cc):
        return pl.ds(pl.multiple_of((xx * nr + yy * 2 + cc) * n, n), n)

    arrays = [part_ref, gpart_ref]
    places = [(x, y), (1 - x, y), (x, 1 - y), (1 - x, 1 - y)]

    core = [[remote(arrays[a].at[rows(*places[k], 1 - c)], cbuf.at[a, k], cs.at[a, k], cr.at[a, k], cp) for k in range(4)] for a in range(2)]
    order = [(0, 1), (0, 3), (1, 2), (1, 3), (0, 2), (1, 1), (0, 0), (1, 0)]
    for a, k in order:
        core[a][k].start()

    def chip_sum(a, k):
        core[a][k].wait_recv()
        cbuf[a, k] = cbuf[a, k] + arrays[a][rows(*places[k], c), :]

    across = [xp, yp]
    far = [1, 2]
    one = [[None, None], [None, None]]
    for a in range(2):
        for j, k in enumerate([far[a], 3]):
            one[a][j] = remote(cbuf.at[a, k], b1.at[a, j], s1s.at[a, j], s1r.at[a, j], across[a])
    for a, k in order[:4]:
        chip_sum(a, k)
        one[a][0 if k == far[a] else 1].start()
    for a, k in order[4:]:
        chip_sum(a, k)
    two = []
    for a in range(2):
        k = far[1 - a]
        one[a][1].wait_recv()
        b1[a, 1] = b1[a, 1] + cbuf[a, k]
        two.append(remote(b1.at[a, 1], b2.at[a], s2s.at[a], s2r.at[a], across[1 - a]))
        two[a].start()
    for a in range(2):
        one[a][0].wait_recv()
        cbuf[a, 0] = cbuf[a, 0] + b1[a, 0]
    hid = both_ref[0].astype(f32)
    mean, inv = stat_ref[:, 0:1], stat_ref[:, 1:2]
    xhat = (hid - mean) * inv
    two[1].wait_recv()
    gn = cbuf[1, 0] + b2[1]
    gnx = gn * xhat
    g = gn * gain_ref[...]
    lane = lax.broadcasted_iota(jnp.int32, (n, 128), 1)
    sums = jnp.where(lane == 0, jnp.sum(g, axis=1, keepdims=True), jnp.sum(g * xhat, axis=1, keepdims=True))
    zbuf[z] = sums.T[:8]
    line = lax.broadcasted_iota(jnp.int32, (8, dz), 0)
    vbuf[me] = jnp.where(
        line == 0, jnp.sum(gnx, axis=0, keepdims=True), jnp.where(line == 1, jnp.sum(gn, axis=0, keepdims=True), 0.0)
    )
    zc = [remote(zbuf.at[z], zbuf.at[z], zs.at[k], zr.at[k], w) for k, w in enumerate(along_z)]
    for copy in zc:
        copy.start()
    vc = [remote(vbuf.at[me], vbuf.at[me], vs.at[k], vr.at[k], w) for k, w in enumerate(plane)]
    for copy in vc:
        copy.start()
    two[0].wait_recv()
    out_ref[...] = (hid + (cbuf[0, 0] + b2[0]) + bias_ref[...]).astype(bf16)
    for copy in zc:
        copy.wait()
    total = zbuf[0]
    for k in range(1, nc):
        total += zbuf[k]
    both = jnp.concatenate([total] * (128 // 8), axis=0).T
    gin_ref[...] = both_ref[1].astype(f32) + inv * (g - both[:, 0:1] / D - xhat * (both[:, 1:2] / D))
    for copy in vc:
        copy.wait()
    total = vbuf[0]
    for k in range(1, npl):
        total += vbuf[k]
    vec_ref[...] = total
    for a, k in order:
        core[a][k].wait_send()
    for a in range(2):
        one[a][0].wait_send()
        one[a][1].wait_send()
        two[a].wait_send()


def attn_kernel(
    pair_ref, wq_ref, wd_ref, bq_ref, small_ref,
    normed_ref, stat_ref, part_ref, gpart_ref, dwq_ref, dwd_ref, dbq_ref, dob_ref,
):
    s = pl.program_id(0)
    z = lax.axis_index("col")
    nz, aw, dz = wd_ref.shape
    seq, D = normed_ref.shape
    heads = aw // HEAD_DIM
    local = pl.ds(pl.multiple_of(z * dz, dz), dz)
    cot_ref = pair_ref.at[1]

    hid = pair_ref[0].astype(f32)
    mean = jnp.sum(hid, axis=1, keepdims=True) / D
    cen = hid - mean
    inv = lax.rsqrt(jnp.sum(cen * cen, axis=1, keepdims=True) / D + epsilon)
    for i in range(nz):
        cols = slice(i * dz, (i + 1) * dz)
        xhat = cen[:, cols] * inv
        normed_ref[:, cols] = (xhat * small_ref[i, 0:1, :dz] + small_ref[i, 1:2, :dz]).astype(bf16)
    lane = lax.broadcasted_iota(jnp.int32, stat_ref.shape, 1)
    stat_ref[...] = jnp.where(lane == 0, mean, inv)

    rows = lax.broadcasted_iota(jnp.int32, (seq, seq), 0)
    cols = lax.broadcasted_iota(jnp.int32, (seq, seq), 1)
    srow = small_ref[s, 2:3, :seq]
    scol = jnp.broadcast_to(srow, (8, seq)).T[:, 0:1]
    same = scol == srow
    allowed = same & (rows >= cols)
    place = jnp.sum(jnp.where(same & (rows < cols), 1.0, 0.0), axis=0, keepdims=True)
    hw = ROT // 2
    freq = lax.broadcasted_iota(jnp.int32, (hw, seq), 0).astype(f32)
    angle = place * jnp.exp(freq * (-2.0 * math.log(10000.0) / ROT))
    cosine, sine = jnp.cos(angle), jnp.sin(angle)
    zero = jnp.zeros((hw, seq), f32)
    rest = jnp.zeros((HEAD_DIM - ROT, seq), f32)
    wide = lambda ts: jnp.concatenate([jnp.concatenate(ts * 2, axis=0).T] * (aw // 128), axis=1)
    own = wide([cosine, cosine, rest + 1.0])
    above = wide([-sine, zero, rest])
    below = wide([zero, sine, rest])

    def rot(t):
        return t * own + pltpu.roll(t, aw - ROT // 2, 1) * above + pltpu.roll(t, ROT // 2, 1) * below

    def unrot(t):
        return t * own - pltpu.roll(t, aw - ROT // 2, 1) * above - pltpu.roll(t, ROT // 2, 1) * below

    proj = dot(normed_ref[...], wq_ref[...], 1, 0) + bq_ref[...]
    q = rot(proj[:, :aw]).astype(bf16)
    k = rot(proj[:, aw : 2 * aw]).astype(bf16)
    v = proj[:, 2 * aw :].astype(bf16)
    gm = jnp.zeros((seq, aw), f32)
    for i in range(nz):
        gm += dot(cot_ref[:, i * dz : (i + 1) * dz], wd_ref[i], 1, 1)
    gm = gm.astype(bf16)
    head_of = lax.broadcasted_iota(jnp.int32, (seq, aw), 1) // HEAD_DIM
    scale = HEAD_DIM ** (-0.5)
    mixed = jnp.zeros((seq, aw), f32)
    gq = jnp.zeros((seq, aw), f32)
    gk = jnp.zeros((seq, aw), f32)
    gv = jnp.zeros((seq, aw), f32)
    zero = jnp.zeros((seq, aw), bf16)
    for h in range(heads):
        mine = head_of == h
        qh = jnp.where(mine, q, zero)
        kh = jnp.where(mine, k, zero)
        vh = jnp.where(mine, v, zero)
        gh = jnp.where(mine, gm, zero)
        scores = jnp.where(allowed, dot(qh, k, 1, 1) * scale, masked_score)
        peak = jnp.max(scores, axis=1, keepdims=True)
        ex = jnp.exp(scores - peak)
        soft = ex * (1.0 / jnp.sum(ex, axis=1, keepdims=True))
        probs = soft.astype(bf16)
        mixed += dot(probs, vh, 1, 0)
        gp = dot(gh, v, 1, 1)
        centre = jnp.sum(soft * gp, axis=1, keepdims=True)
        gs = (soft * (gp - centre)).astype(bf16)
        gq += dot(gs, kh, 1, 0)
        gk += dot(gs, qh, 0, 0)
        gv += dot(probs, gh, 0, 0)
    mixed = mixed.astype(bf16)
    g = jnp.concatenate([unrot(gq * scale), unrot(gk * scale), gv], axis=1).astype(bf16)
    cot_loc = cot_ref[:, local]
    normed_loc = normed_ref[:, local]
    part_ref[...] = dot(mixed, wd_ref[z], 1, 0)
    gpart_ref[...] = dot(g, wq_ref[local, :], 1, 1)

    @pl.when(s == 0)
    def _():
        dwq_ref[...] = jnp.zeros_like(dwq_ref)
        dwd_ref[...] = jnp.zeros_like(dwd_ref)
        dbq_ref[...] = jnp.zeros_like(dbq_ref)
        dob_ref[...] = jnp.zeros_like(dob_ref)

    dob_ref[...] += jnp.sum(cot_loc.astype(f32), axis=0, keepdims=True)
    dwq_ref[...] += dot(normed_loc, g, 0, 0)
    dwd_ref[...] += dot(mixed, cot_loc, 0, 0)
    dbq_ref[...] += jnp.sum(g.astype(f32), axis=0, keepdims=True)


def attend(normed_ref, cot_ref, local, z, nz, wq, wd, bq_ref, srow, part_ref, gpart_ref, dwq_ref, dwd_ref, dbq_ref):
    seq = normed_ref.shape[0]
    aw, dz = dwd_ref.shape
    heads = aw // HEAD_DIM
    rows = lax.broadcasted_iota(jnp.int32, (seq, seq), 0)
    cols = lax.broadcasted_iota(jnp.int32, (seq, seq), 1)
    scol = jnp.broadcast_to(srow, (8, seq)).T[:, 0:1]
    same = scol == srow
    allowed = same & (rows >= cols)
    place = jnp.sum(jnp.where(same & (rows < cols), 1.0, 0.0), axis=0, keepdims=True)
    hw = ROT // 2
    freq = lax.broadcasted_iota(jnp.int32, (hw, seq), 0).astype(f32)
    angle = place * jnp.exp(freq * (-2.0 * math.log(10000.0) / ROT))
    cosine, sine = jnp.cos(angle), jnp.sin(angle)
    zero = jnp.zeros((hw, seq), f32)
    rest = jnp.zeros((HEAD_DIM - ROT, seq), f32)
    wide = lambda ts: jnp.concatenate([jnp.concatenate(ts * 2, axis=0).T] * (aw // 128), axis=1)
    own = wide([cosine, cosine, rest + 1.0])
    above = wide([-sine, zero, rest])
    below = wide([zero, sine, rest])

    def rot(t):
        return t * own + pltpu.roll(t, aw - hw, 1) * above + pltpu.roll(t, hw, 1) * below

    def unrot(t):
        return t * own - pltpu.roll(t, aw - hw, 1) * above - pltpu.roll(t, hw, 1) * below

    def across(ref, w, axis, width):
        total = jnp.zeros((seq, width), f32)
        for i in range(nz):
            total += dot(ref[:, i * dz : (i + 1) * dz], w(i)[...], 1, axis)
        return total

    proj = across(normed_ref, wq, 0, 3 * aw) + bq_ref[...]
    q = rot(proj[:, :aw]).astype(bf16)
    k = rot(proj[:, aw : 2 * aw]).astype(bf16)
    v = proj[:, 2 * aw :].astype(bf16)
    gm = across(cot_ref, wd, 1, aw).astype(bf16)
    head_of = lax.broadcasted_iota(jnp.int32, (seq, aw), 1) // HEAD_DIM
    scale = HEAD_DIM ** (-0.5)
    mixed = jnp.zeros((seq, aw), f32)
    gq = jnp.zeros((seq, aw), f32)
    gk = jnp.zeros((seq, aw), f32)
    gv = jnp.zeros((seq, aw), f32)
    none = jnp.zeros((seq, aw), bf16)
    for h in range(heads):
        mine = head_of == h
        qh = jnp.where(mine, q, none)
        kh = jnp.where(mine, k, none)
        vh = jnp.where(mine, v, none)
        gh = jnp.where(mine, gm, none)
        scores = jnp.where(allowed, dot(qh, k, 1, 1) * scale, masked_score)
        peak = jnp.max(scores, axis=1, keepdims=True)
        ex = jnp.exp(scores - peak)
        soft = ex * (1.0 / jnp.sum(ex, axis=1, keepdims=True))
        probs = soft.astype(bf16)
        mixed += dot(probs, vh, 1, 0)
        gp = dot(gh, v, 1, 1)
        centre = jnp.sum(soft * gp, axis=1, keepdims=True)
        gs = (soft * (gp - centre)).astype(bf16)
        gq += dot(gs, kh, 1, 0)
        gk += dot(gs, qh, 0, 0)
        gv += dot(probs, gh, 0, 0)
    mixed = mixed.astype(bf16)
    g = jnp.concatenate([unrot(gq * scale), unrot(gk * scale), gv], axis=1).astype(bf16)
    part_ref[...] = dot(mixed, wd(z)[...], 1, 0)
    gpart_ref[...] = dot(g, wq(z)[...], 1, 1)
    dwq_ref[...] += dot(normed_ref[:, local], g, 0, 0)
    dwd_ref[...] += dot(mixed, cot_ref[:, local], 0, 0)
    dbq_ref[...] += jnp.sum(g.astype(f32), axis=0, keepdims=True)


def hidden(normed_ref, cot_ref, local, z, nz, w1, w2, b1, part_ref, gpart_ref, dw1_ref, dw2_ref, db1_ref):
    tb = normed_ref.shape[0]
    dz, fc = dw1_ref.shape
    u = jnp.zeros((tb, fc), f32)
    ga = jnp.zeros((tb, fc), f32)
    for i in range(nz):
        cols = slice(i * dz, (i + 1) * dz)
        u += dot(normed_ref[:, cols], w1(i)[...], 1, 0)
        ga += dot(cot_ref[:, cols], w2(i)[...], 1, 1)
    u += b1
    ga = ga.astype(bf16).astype(f32)
    u2 = u * u
    t = jnp.tanh(C0 * (u + C1 * (u2 * u)))
    cdf = 0.5 * (1.0 + t)
    act = (u * cdf).astype(bf16)
    slope = cdf + (0.5 * u) * (1.0 - t * t) * (C0 * (1.0 + (3.0 * C1) * u2))
    gh = (slope * ga).astype(bf16)
    part_ref[...] += dot(act, w2(z)[...], 1, 0)
    gpart_ref[...] += dot(gh, w1(z)[...], 1, 1)
    dw1_ref[...] += dot(normed_ref[:, local], gh, 0, 0)
    dw2_ref[...] += dot(act, cot_ref[:, local], 0, 0)
    db1_ref[...] += jnp.sum(gh.astype(f32), axis=0, keepdims=True)


def layer_kernel(
    both_ref, wq_ref, wd_ref, w1_ref, w2_ref, bq_ref, b1_ref, small_ref, gain_ref, bias_ref,
    out_ref, gin_ref, vec_ref, gb_ref, gq_ref, gd_ref, g1_ref, g2_ref,
    tok, wq_s, wd_s, w1_s, w2_s, part, gpart, dq, dd, d1, d2, stat, smalls, cbuf, ring1, ring2, zbuf, vbuf,
    ksem, zs, zr, xs, xr, ys, yr, cs, cr, as_, ar, ms, mr, ts, tr, ds, dr, ls, bs, br,
    rcs, rcr, r1s, r1r, r2s, r2r, zbs, zbr, vbs, vbr,
):
    _, n, dz = both_ref.shape
    nd, nr, nc = lax.axis_size("dp"), lax.axis_size("row"), lax.axis_size("col")
    _, T, D = tok.shape
    nj, _, _, fc = w1_s.shape
    aw, fw = wd_s.shape[1], nj * fc
    ns, npl = nd * nc, nd * nr
    seq = n
    x, r, z = lax.axis_index("dp"), lax.axis_index("row"), lax.axis_index("col")
    y, c = r // 2, lax.rem(r, 2)
    rp, rc = lax.rem(r + 2, nr), r + 1 - 2 * c
    rcp = lax.rem(rc + 2, nr)
    xp, yp, cp = {"dp": 1 - x}, {"row": rp}, {"row": rc}
    beside = [{"col": z - 1}, {"col": z + 1}]
    line, plane = [], []
    for k in range(1, ns):
        o = lax.rem(x * nc + z + k, ns)
        line.append({"dp": o // nc, "col": lax.rem(o, nc)})
    me = x * nr + r
    for k in range(1, npl):
        o = lax.rem(me + k, npl)
        plane.append({"dp": o // nr, "row": lax.rem(o, nr)})
    along = [{"col": lax.rem(z + k, nc)} for k in range(1, nc)]
    greet([(True, w) for w in line + plane])

    local = pl.ds(pl.multiple_of(z * dz, dz), dz)
    at = lambda i, size: pl.ds(pl.multiple_of(i * size, size), size)

    def item(g, zz):
        return tok.at[:, at(g, n), at(zz, dz)]

    mine = [x * nr + r, (1 - x) * nr + r, x * nr + rp, (1 - x) * nr + rp]
    theirs = [x * nr + rc, (1 - x) * nr + rc, x * nr + rcp, (1 - x) * nr + rcp]

    def each(body, steps=range(nc)):
        for s in steps:
            for zz in [z] if s == 0 else [z - s, z + s]:
                if s == 0:
                    body(s, zz)
                else:

                    @pl.when((zz >= 0) & (zz < nc))
                    def _():
                        body(s, zz)

    def outward(zz, send):
        @pl.when((zz >= z) & (z > 0))
        def _():
            send(0)

        @pl.when((zz <= z) & (z < nc - 1))
        def _():
            send(1)

    def tokens(d, s, zz):
        src = both_ref if s == 0 else item(mine[0], zz)
        return remote(src, item(mine[0], zz), zs.at[d, zz], zr.at[zz], beside[d])

    wd_own = wd_ref.at[at(x, aw), :]
    w1_own = lambda j: w1_ref.at[:, at(x * nj + j, fc)]
    w2_own = lambda j: w2_ref.at[at(x * nj + j, fc), :]

    def pieces(j, own, zz):
        if j < 0:
            a, b = wq_s.at[zz], wd_s.at[zz]
            return [(wq_ref if own else a, a), (wd_own if own else b, b)]
        a, b = w1_s.at[j, zz], w2_s.at[j, zz]
        return [(w1_own(j) if own else a, a), (w2_own(j) if own else b, b)]

    def weights(j, d, own, zz):
        sems = [(as_.at[k, d, zz], ar.at[k, zz]) if j < 0 else (ms.at[k, d, j, zz], mr.at[k, j, zz]) for k in range(2)]
        return [remote(a, b, *sems[k], beside[d]) for k, (a, b) in enumerate(pieces(j, own, zz))]

    def pass_weights(j, steps, go=True):
        def body(s, zz):
            if s > 0:
                for copy in weights(j, 0, False, zz):
                    copy.wait_recv()

            def send(d):
                for copy in weights(j, d, s == 0, zz):
                    copy.start()

            if go:
                outward(zz, send)

        each(body, steps)

    def to(sems, peer):
        return lambda k, src, g, zz: remote(src, item(g, zz), sems[0].at[k, zz], sems[1].at[k, zz], peer)

    to_x, to_y, to_core = to((xs, xr), xp), to((ys, yr), yp), to((cs, cr), cp)

    def first(s, zz):
        if s > 0:
            tokens(0, s, zz).wait_recv()
        outward(zz, lambda d: tokens(d, s, zz).start())
        src = both_ref if s == 0 else item(mine[0], zz)
        for send in (to_x, to_y, to_core):
            send(0, src, mine[0], zz).start()

    def second(s, zz):
        even = lax.rem(zz, 2) == 0
        a, b = item(mine[1], zz), item(mine[2], zz)
        to_x(0, a, mine[1], zz).wait_recv()

        @pl.when(even)
        def _():
            to_y(1, a, mine[1], zz).start()

        to_core(1, a, mine[1], zz).start()
        to_y(0, b, mine[2], zz).wait_recv()

        @pl.when(jnp.logical_not(even))
        def _():
            to_x(1, b, mine[2], zz).start()

        to_core(2, b, mine[2], zz).start()

    def third(s, zz):
        even = lax.rem(zz, 2) == 0
        d = item(mine[3], zz)

        @pl.when(even)
        def _():
            to_y(1, d, mine[3], zz).wait_recv()

        @pl.when(jnp.logical_not(even))
        def _():
            to_x(1, d, mine[3], zz).wait_recv()

        to_core(3, d, mine[3], zz).start()

    def fourth(s, zz):
        even = lax.rem(zz, 2) == 0
        for k in range(4):
            to_core(k, both_ref, theirs[k], zz).wait()
        to_x(0, both_ref, mine[0], zz).wait_send()
        to_y(0, both_ref, mine[0], zz).wait_send()

        @pl.when(even)
        def _():
            to_y(1, both_ref, mine[1], zz).wait_send()

        @pl.when(jnp.logical_not(even))
        def _():
            to_x(1, both_ref, mine[2], zz).wait_send()

        outward(zz, lambda d: tokens(d, 0, zz).wait_send())

    keeps = [(both_ref, item(mine[0], z)), (small_ref, smalls.at[x * nc + z]), *pieces(-1, True, z)]
    for j in range(nj):
        keeps += pieces(j, True, z)
    keeps = [pltpu.make_async_copy(a, b, ksem.at[k]) for k, (a, b) in enumerate(keeps)]
    tiny = [remote(small_ref, smalls.at[x * nc + z], ts.at[k], tr.at[k], w) for k, w in enumerate(line)]

    each(first, range(1))
    for copy in tiny + keeps:
        copy.start()
    each(first, range(1, nc))
    pass_weights(-1, range(1))
    each(second)
    pass_weights(-1, range(1, 2))
    pass_weights(0, range(1))
    each(third)
    for copy in keeps + tiny:
        copy.wait()
    each(fourth)

    dq[...] = jnp.zeros_like(dq)
    dd[...] = jnp.zeros_like(dd)
    d1[...] = jnp.zeros_like(d1)
    d2[...] = jnp.zeros_like(d2)
    gb_ref[x] = jnp.zeros(gb_ref.shape[1:], f32)
    vec_ref[...] = jnp.zeros_like(vec_ref)

    def norm(s, _):
        rows = at(s, seq)
        hid = tok[0, rows, :].astype(f32)
        mean = jnp.sum(hid, axis=1, keepdims=True) / D
        cen = hid - mean
        inv = lax.rsqrt(jnp.sum(cen * cen, axis=1, keepdims=True) / D + epsilon)
        for i in range(nc):
            cols = slice(i * dz, (i + 1) * dz)
            xhat = cen[:, cols] * inv
            tok[0, rows, cols] = (xhat * smalls[i, 0:1, :dz] + smalls[i, 1:2, :dz]).astype(bf16)
        lane = lax.broadcasted_iota(jnp.int32, (seq, 128), 1)
        stat[rows, :] = jnp.where(lane == 0, mean, inv)
        vec_ref[2:3, :] += jnp.sum(tok[1, rows, local].astype(f32), axis=0, keepdims=True)
        return 0

    lax.fori_loop(0, T // seq, norm, 0)
    pass_weights(-1, range(2, nc - 1))
    pass_weights(-1, range(nc - 1, nc), go=False)
    pass_weights(0, range(1, 2))
    pass_weights(1, range(1))

    def attn(s, _):
        @pl.when(s == 3)
        def _():
            pass_weights(0, range(2, nc - 1))

        @pl.when(s == 6)
        def _():
            pass_weights(1, range(1, 2))

        rows = at(s, seq)
        attend(
            tok.at[0, rows, :], tok.at[1, rows, :], local, z, nc, lambda i: wq_s.at[i], lambda i: wd_s.at[i], bq_ref,
            smalls[s, 2:3, :seq], part.at[rows, :], gpart.at[rows, :], dq, dd, gb_ref.at[x, 0, 0:1, : 3 * aw],
        )
        return 0

    lax.fori_loop(0, T // seq, attn, 0)

    def settle(k, src, dst):
        return [remote(src, dst, ds.at[k], dr.at[k], xp), pltpu.make_async_copy(src, dst, ls.at[k])]

    dqs = [settle(k, dq.at[:, k * aw : (k + 1) * aw], gq_ref.at[k, :, at(x, aw)]) for k in range(3)]
    dense = settle(3, dd, gd_ref.at[at(x, aw), :])

    def mlp_grads(j):
        return settle(4 + 2 * j, d1.at[j], g1_ref.at[:, at(x * nj + j, fc)]) + settle(
            5 + 2 * j, d2.at[j], g2_ref.at[at(x * nj + j, fc), :]
        )

    for copies in dqs + [dense]:
        for copy in copies:
            copy.start()

    arrays = [part, gpart]
    places = [(x, y), (1 - x, y), (x, 1 - y), (1 - x, 1 - y)]
    rows_of = lambda k, cc: at(places[k][0] * nr + places[k][1] * 2 + cc, n)
    core = [
        [remote(arrays[a].at[rows_of(k, 1 - c), :], cbuf.at[a, k], rcs.at[a, k], rcr.at[a, k], cp) for k in range(4)]
        for a in range(2)
    ]
    nb = 4
    turn = [3, 1, 2, 0]
    last = nj - 1
    sends = {0: [(2, 0)], 4: [(1, 2), (3, 0)], 6: [(2, 1)], 8: [(2, 2)], 10: [(3, 1)], 12: [(3, 2)]}

    def mlp(t, _):
        j, b = t // nb, lax.rem(t, nb)
        for k, todo in sends.items():

            @pl.when(t == k)
            def _():
                for jj, s in todo:
                    pass_weights(jj, range(s, s + 1))
                if k % nb == 0:
                    pass_weights(k // nb, range(nc - 1, nc), go=False)

        xx = jnp.where((b == 0) | (b == 1), 1 - x, x)
        yy = jnp.where((b == 0) | (b == 2), 1 - y, y)
        rows = at(xx * (nr // 2) + yy, 2 * n)
        hidden(
            tok.at[0, rows, :], tok.at[1, rows, :], local, z, nc, lambda i: w1_s.at[j, i], lambda i: w2_s.at[j, i],
            b1_ref[j], part.at[rows, :], gpart.at[rows, :], d1.at[j], d2.at[j], gb_ref.at[x, j + 1, 0:1, :fc],
        )
        for k in range(nb):

            @pl.when(t == last * nb + k)
            def _():
                core[0][turn[k]].start()
                core[1][turn[k]].start()

        for jj in range(nj):

            @pl.when(t == jj * nb + nb - 1)
            def _():
                if jj < last:
                    for copy in mlp_grads(jj):
                        copy.start()

        return 0

    lax.fori_loop(0, nj * nb, mlp, 0)

    def chip_sum(a, k):
        core[a][k].wait_recv()
        cbuf[a, k] = cbuf[a, k] + arrays[a][rows_of(k, c), :]

    over = [xp, yp]
    far = [1, 2]
    one = [
        [remote(cbuf.at[a, k], ring1.at[a, i], r1s.at[a, i], r1r.at[a, i], over[a]) for i, k in enumerate([far[a], 3])]
        for a in range(2)
    ]
    for i in (1, 0):
        for a in range(2):
            chip_sum(a, [far[a], 3][i])
            one[a][i].start()
    for copy in mlp_grads(last):
        copy.start()
    bias_copy = remote(gb_ref.at[x], gb_ref.at[x], bs, br, xp)
    bias_copy.start()
    for a in range(2):
        chip_sum(a, far[1 - a])
    for a in range(2):
        chip_sum(a, 0)
    two = []
    for a in range(2):
        one[a][1].wait_recv()
        ring1[a, 1] = ring1[a, 1] + cbuf[a, far[1 - a]]
        two.append(remote(ring1.at[a, 1], ring2.at[a], r2s.at[a], r2r.at[a], over[1 - a]))
        two[a].start()
    for a in range(2):
        one[a][0].wait_recv()
        cbuf[a, 0] = cbuf[a, 0] + ring1[a, 0]
    hid = both_ref[0].astype(f32)
    ours = stat[at(me, n), :]
    mean, inv = ours[:, 0:1], ours[:, 1:2]
    xhat = (hid - mean) * inv
    two[1].wait_recv()
    gn = cbuf[1, 0] + ring2[1]
    g = gn * gain_ref[...]
    lane = lax.broadcasted_iota(jnp.int32, (n, 128), 1)
    sums = jnp.where(lane == 0, jnp.sum(g, axis=1, keepdims=True), jnp.sum(g * xhat, axis=1, keepdims=True))
    zbuf[z] = sums.T[:8]
    zc = [remote(zbuf.at[z], zbuf.at[z], zbs.at[k], zbr.at[k], w) for k, w in enumerate(along)]
    for copy in zc:
        copy.start()
    which = lax.broadcasted_iota(jnp.int32, (8, dz), 0)
    vbuf[me] = jnp.where(
        which == 0,
        jnp.sum(gn * xhat, axis=0, keepdims=True),
        jnp.where(which == 1, jnp.sum(gn, axis=0, keepdims=True), 0.0),
    )
    vc = [remote(vbuf.at[me], vbuf.at[me], vbs.at[k], vbr.at[k], w) for k, w in enumerate(plane)]
    for copy in vc:
        copy.start()
    two[0].wait_recv()
    out_ref[...] = (hid + (cbuf[0, 0] + ring2[0]) + bias_ref[...]).astype(bf16)
    for copy in zc:
        copy.wait()
    total = zbuf[0]
    for k in range(1, nc):
        total += zbuf[k]
    total = jnp.concatenate([total] * (128 // 8), axis=0).T
    gin_ref[...] = both_ref[1].astype(f32) + inv * (g - total[:, 0:1] / D - xhat * (total[:, 1:2] / D))
    for copy in vc:
        copy.wait()
    total = vbuf[0]
    for k in range(1, npl):
        total += vbuf[k]
    vec_ref[0:2, :] = total[0:2]

    bias_copy.wait()
    for a in range(2):
        for k in range(4):
            core[a][k].wait_send()
        one[a][0].wait_send()
        one[a][1].wait_send()
        two[a].wait_send()
    for copies in dqs + [dense] + [mlp_grads(j) for j in range(nj)]:
        for copy in copies:
            copy.wait()

    def sent(s, zz):
        def wait(d):
            for j in range(-1, nj):
                for copy in weights(j, d, True, zz):
                    copy.wait_send()

        outward(zz, wait)

    each(sent)


def mlp_kernel(joint, normed_ref, cot_ref, *refs):
    if joint:
        w_ref, *refs = refs
        w1 = lambda i: w_ref.at[i, 0]
        w2 = lambda i: w_ref.at[i, 1]
    else:
        w1_ref, w2_ref, *refs = refs
        w1 = lambda i: w1_ref.at[i]
        w2 = lambda i: w2_ref.at[i]
    b1_ref, part_in, gpart_in, part_ref, gpart_ref, dw1_ref, dw2_ref, db1_ref, act_s, gh_s = refs
    s = pl.program_id(0)
    z = lax.axis_index("col")
    dz, fw = dw1_ref.shape
    nz = normed_ref.shape[1] // dz
    tb = normed_ref.shape[0]
    local = pl.ds(pl.multiple_of(z * dz, dz), dz)
    fb = 256
    for j in range(fw // fb):
        fs = slice(j * fb, (j + 1) * fb)
        u = b1_ref[:, fs] + jnp.zeros((tb, fb), f32)
        for i in range(nz):
            u += dot(normed_ref[:, i * dz : (i + 1) * dz], w1(i)[:, fs], 1, 0)
        ga = jnp.zeros((tb, fb), f32)
        for i in range(nz):
            ga += dot(cot_ref[:, i * dz : (i + 1) * dz], w2(i)[fs, :], 1, 1)
        ga = ga.astype(bf16).astype(f32)
        u2 = u * u
        t = jnp.tanh(C0 * (u + C1 * (u2 * u)))
        cdf = 0.5 * (1.0 + t)
        act_s[:, fs] = (u * cdf).astype(bf16)
        slope = cdf + (0.5 * u) * (1.0 - t * t) * (C0 * (1.0 + (3.0 * C1) * u2))
        gh_s[:, fs] = (slope * ga).astype(bf16)
    act, gh = act_s[...], gh_s[...]
    cot_loc = cot_ref[:, local]
    normed_loc = normed_ref[:, local]
    part_ref[...] = part_in[...] + dot(act, w2(z)[...], 1, 0)
    gpart_ref[...] = gpart_in[...] + dot(gh, w1(z)[...], 1, 1)

    @pl.when(s == 0)
    def _():
        dw1_ref[...] = jnp.zeros_like(dw1_ref)
        dw2_ref[...] = jnp.zeros_like(dw2_ref)
        db1_ref[...] = jnp.zeros_like(db1_ref)

    dw1_ref[...] += dot(normed_loc, gh, 0, 0)
    dw2_ref[...] += dot(act, cot_loc, 0, 0)
    db1_ref[...] += jnp.sum(gh.astype(f32), axis=0, keepdims=True)


def shape(s, d):
    return jax.ShapeDtypeStruct(s, d)


def whole(s):
    return pl.BlockSpec(s, lambda i: (0,) * len(s))


def shards_apart(hidden_in, cotangent, segment_ids, w_qkv, b_qkv, w_fc1, b_fc1, w_dense, w_fc2, out_bias, ln_gain, ln_shift):
    nd, nr, nc = lax.axis_size("dp"), lax.axis_size("row"), lax.axis_size("col")
    x, z = lax.axis_index("dp"), lax.axis_index("col")
    seq_len = segment_ids.shape[1]
    nloc, dz = hidden_in.shape
    D = dz * nc
    T = nloc * nd * nr
    nseq = T // seq_len
    aw = w_qkv.shape[2] // nd
    fw = w_fc1.shape[1] // nd
    half = lambda w, n, axis: lax.dynamic_slice_in_dim(w, x * n, n, axis)

    both = jnp.stack([hidden_in, cotangent])
    dma = pltpu.SemaphoreType.DMA
    wq = half(w_qkv, aw, 2).reshape(dz, 3 * aw)
    bq = half(b_qkv, aw, 1).astype(f32).reshape(1, 3 * aw)
    b1 = half(b_fc1, fw, 0).astype(f32).reshape(1, fw)
    nchunk = 2
    fc = fw // nchunk
    chunks = []
    for i in range(nchunk):
        w1 = lax.dynamic_slice_in_dim(w_fc1, x * fw + i * fc, fc, 1)
        w2 = lax.dynamic_slice_in_dim(w_fc2, x * fw + i * fc, fc, 0)
        if fc == dz:
            chunks.append([lax.all_gather(jnp.stack([w1, w2]), "col", axis=0)])
        else:
            chunks.append([lax.all_gather(w1, "col", axis=0), lax.all_gather(w2, "col", axis=0)])
    sw = max(dz, seq_len)
    line = lambda a: jnp.pad(a.astype(f32), ((0, 0), (0, sw - a.shape[1])))
    small = jnp.concatenate(
        [line(ln_gain[None]), line(ln_shift[None]), line(segment_ids), jnp.zeros((5, sw), f32)], axis=0
    )
    hbm = pl.BlockSpec(memory_space=pl.ANY)
    ns = nd * nc
    pair, wq_all, wd_all, small_all = pl.pallas_call(
        gather_kernel,
        in_specs=[hbm] * 4,
        out_specs=[hbm] * 4,
        out_shape=[shape((2, T, D), bf16), shape((D, 3 * aw), bf16), shape((nc, aw, dz), bf16), shape((ns, 8, sw), f32)],
        scratch_shapes=[
            dma((4,)), dma((2, nc)), dma((nc,)), dma((2, nc)), dma((2, nc)), dma((2, nc)), dma((2, nc)), dma((4, nc)), dma((4, nc)),
            dma((2, 2, nc)), dma((2, nc)), dma((ns - 1,)), dma((ns - 1,)),
        ],
        compiler_params=pltpu.CompilerParams(collective_id=0, has_side_effects=True),
        name="gather",
    )(both, wq, w_dense, small)

    blk = lambda n, w: pl.BlockSpec((n, w), lambda i: (i, 0))
    normed, stat, part, gpart, dwq, dwd, dbq, dob = pl.pallas_call(
        attn_kernel,
        grid=(nseq,),
        in_specs=[
            pl.BlockSpec((2, seq_len, D), lambda i: (0, i, 0)), whole((D, 3 * aw)), whole((nc, aw, dz)), whole((1, 3 * aw)),
            whole((ns, 8, sw)),
        ],
        out_specs=[
            blk(seq_len, D), blk(seq_len, 128), blk(seq_len, dz), blk(seq_len, dz),
            whole((dz, 3 * aw)), whole((aw, dz)), whole((1, 3 * aw)), whole((1, dz)),
        ],
        out_shape=[
            shape((T, D), bf16), shape((T, 128), f32), shape((T, dz), f32), shape((T, dz), f32),
            shape((dz, 3 * aw), f32), shape((aw, dz), f32), shape((1, 3 * aw), f32), shape((1, dz), f32),
        ],
        name="attn",
    )(pair, wq_all, wd_all, bq, small_all)
    swap = lambda a: lax.ppermute(a, "dp", [(i, nd - 1 - i) for i in range(nd)])

    def join(a, axis):
        b = swap(a)
        return jnp.concatenate([jnp.where(x == 0, a, b), jnp.where(x == 0, b, a)], axis=axis)

    def put(into, a, i, axis):
        at = lambda who: [0] * axis + [who * fw + i * fc] + [0] * (1 - axis)
        into = lax.dynamic_update_slice(into, a, at(x))
        return lax.dynamic_update_slice(into, swap(a), at(1 - x))

    g_qkv = join(dwq.reshape(dz, 3, aw), 2)
    g_bq = join(dbq.reshape(3, aw), 1)
    g_dense = join(dwd, 0)
    g_fc1 = jnp.zeros((dz, nd * fw), f32)
    g_fc2 = jnp.zeros((nd * fw, dz), f32)
    g_b1 = jnp.zeros((1, nd * fw), f32)

    tb = 512
    cot_blk = lambda n: pl.BlockSpec((None, n, D), lambda i: (1, i, 0))
    if len(chunks[0]) == 1:
        w_specs = [whole((nc, 2, dz, fc))]
    else:
        w_specs = [whole((nc, dz, fc)), whole((nc, fc, dz))]
    for i in range(nchunk):
        part, gpart, a, b, c = pl.pallas_call(
            functools.partial(mlp_kernel, len(chunks[i]) == 1),
            grid=(T // tb,),
            in_specs=[
                blk(tb, D), cot_blk(tb), *w_specs, whole((1, fc)), blk(tb, dz), blk(tb, dz),
            ],
            out_specs=[blk(tb, dz), blk(tb, dz), whole((dz, fc)), whole((fc, dz)), whole((1, fc))],
            out_shape=[shape((T, dz), f32), shape((T, dz), f32), shape((dz, fc), f32), shape((fc, dz), f32), shape((1, fc), f32)],
            scratch_shapes=[pltpu.VMEM((tb, fc), bf16), pltpu.VMEM((tb, fc), bf16)],
            name="mlp",
        )(normed, pair, *chunks[i], b1[:, i * fc : (i + 1) * fc], part, gpart)
        g_fc1 = put(g_fc1, a, i, 1)
        g_fc2 = put(g_fc2, b, i, 0)
        g_b1 = put(g_b1, c, i, 1)

    me = lax.axis_index(("dp", "row"))
    stat_l = lax.dynamic_slice_in_dim(stat, me * nloc, nloc, 0)
    vmem = pl.BlockSpec(memory_space=pltpu.VMEM)
    npl = nd * nr
    output, grad_input, vec = pl.pallas_call(
        functools.partial(tail_kernel, D),
        in_specs=[vmem] * 6,
        out_specs=[vmem] * 3,
        out_shape=[shape((nloc, dz), bf16), shape((nloc, dz), f32), shape((8, dz), f32)],
        scratch_shapes=[
            pltpu.VMEM((2, 4, nloc, dz), f32), pltpu.VMEM((2, 2, nloc, dz), f32), pltpu.VMEM((2, nloc, dz), f32),
            pltpu.VMEM((nc, 8, nloc), f32), pltpu.VMEM((npl, 8, dz), f32),
            dma((2, 4)), dma((2, 4)), dma((2, 2)), dma((2, 2)), dma((2,)), dma((2,)),
            dma((nc - 1,)), dma((nc - 1,)), dma((npl - 1,)), dma((npl - 1,)),
        ],
        compiler_params=pltpu.CompilerParams(collective_id=1, has_side_effects=True),
        name="tail",
    )(part, gpart, both, stat_l, ln_gain.astype(f32).reshape(1, dz), out_bias.astype(f32).reshape(1, dz))
    return (output, grad_input, g_qkv, g_bq, g_fc1, g_b1[0], g_dense, g_fc2, dob[0], vec[0], vec[1])


def shards_whole(hidden_in, cotangent, segment_ids, w_qkv, b_qkv, w_fc1, b_fc1, w_dense, w_fc2, out_bias, ln_gain, ln_shift):
    nd, nr, nc = lax.axis_size("dp"), lax.axis_size("row"), lax.axis_size("col")
    x = lax.axis_index("dp")
    n, dz = hidden_in.shape
    seq = segment_ids.shape[1]
    D, T = dz * nc, n * nd * nr
    aw, fw = w_qkv.shape[2] // nd, w_fc1.shape[1] // nd
    nj = 4
    fc = fw // nj
    ns, npl = nd * nc, nd * nr
    half = lambda w, size, axis: lax.dynamic_slice_in_dim(w, x * size, size, axis)
    wq = half(w_qkv, aw, 2).reshape(dz, 3 * aw)
    bq = half(b_qkv, aw, 1).astype(f32).reshape(1, 3 * aw)
    b1 = half(b_fc1, fw, 0).astype(f32).reshape(nj, 1, fc)
    sw = max(dz, seq)
    line = lambda a: jnp.pad(a.astype(f32), ((0, 0), (0, sw - a.shape[1])))
    small = jnp.concatenate([line(ln_gain[None]), line(ln_shift[None]), line(segment_ids), jnp.zeros((5, sw), f32)], axis=0)
    hbm, vmem = pl.BlockSpec(memory_space=pl.ANY), pl.BlockSpec(memory_space=pltpu.VMEM)
    dma = pltpu.SemaphoreType.DMA
    v = pltpu.VMEM
    nk = 4 + 2 * nj
    gw = max(3 * aw, fc)
    out, gin, vec, gb, gq, gd, g1, g2 = pl.pallas_call(
        layer_kernel,
        in_specs=[vmem, hbm, hbm, hbm, hbm, vmem, vmem, vmem, vmem, vmem],
        out_specs=[vmem] * 4 + [hbm] * 4,
        out_shape=[
            shape((n, dz), bf16), shape((n, dz), f32), shape((8, dz), f32), shape((nd, nj + 1, 8, gw), f32),
            shape((3, dz, nd * aw), f32), shape((nd * aw, dz), f32), shape((dz, nd * fw), f32), shape((nd * fw, dz), f32),
        ],
        scratch_shapes=[
            v((2, T, D), bf16), v((nc, dz, 3 * aw), bf16), v((nc, aw, dz), bf16),
            v((nj, nc, dz, fc), bf16), v((nj, nc, fc, dz), bf16),
            v((T, dz), f32), v((T, dz), f32), v((dz, 3 * aw), f32), v((aw, dz), f32), v((nj, dz, fc), f32), v((nj, fc, dz), f32),
            v((T, 128), f32), v((ns, 8, sw), f32), v((2, 4, n, dz), f32), v((2, 2, n, dz), f32), v((2, n, dz), f32),
            v((nc, 8, n), f32), v((npl, 8, dz), f32),
            dma((4 + 2 * nj,)), dma((2, nc)), dma((nc,)), dma((2, nc)), dma((2, nc)), dma((2, nc)), dma((2, nc)), dma((4, nc)), dma((4, nc)),
            dma((2, 2, nc)), dma((2, nc)), dma((2, 2, nj, nc)), dma((2, nj, nc)), dma((ns - 1,)), dma((ns - 1,)),
            dma((nk,)), dma((nk,)), dma((nk,)), dma, dma,
            dma((2, 4)), dma((2, 4)), dma((2, 2)), dma((2, 2)), dma((2,)), dma((2,)),
            dma((nc - 1,)), dma((nc - 1,)), dma((npl - 1,)), dma((npl - 1,)),
        ],
        compiler_params=pltpu.CompilerParams(collective_id=0, has_side_effects=True, vmem_limit_bytes=67043328),
        name="layer",
    )(
        jnp.stack([hidden_in, cotangent]), wq, w_dense, w_fc1, w_fc2, bq, b1, small,
        ln_gain.astype(f32).reshape(1, dz), out_bias.astype(f32).reshape(1, dz),
    )
    g_bq = gb[:, 0, 0, : 3 * aw].reshape(nd, 3, aw).transpose(1, 0, 2).reshape(3, nd * aw)
    g_b1 = gb[:, 1:, 0, :fc].reshape(nd * fw)
    return (out, gin, gq.transpose(1, 0, 2), g_bq, g1, g_b1, gd, g2, vec[2], vec[0], vec[1])


def shards(*args):
    n, dz = args[0].shape
    nd, nr, nc = lax.axis_size("dp"), lax.axis_size("row"), lax.axis_size("col")
    tokens = n * nd * nr * dz * nc
    fits = nc == 4 and nd == 2 and nr == 4 and args[2].shape[1] == n and tokens <= 1 << 22
    return (shards_whole if fits else shards_apart)(*args)


def solution(mesh):
    in_specs = (
        P(("dp", "row"), "col"), P(("dp", "row"), "col"), P(("dp", "col"), None), P("col", None, "row"), P(None, "row"),
        P("col", "row"), P("row"), P("row", "col"), P("row", "col"), P("col"), P("col"), P("col"),
    )
    out_specs = (
        P(("dp", "row"), "col"), P(("dp", "row"), "col"), P("col", None, "row"), P(None, "row"), P("col", "row"), P("row"),
        P("row", "col"), P("row", "col"), P("col"), P("col"), P("col"),
    )
    return jax.shard_map(shards, mesh=mesh, in_specs=in_specs, out_specs=out_specs, check_vma=False)
```
